32 devices in a mesh: row: 16 (over z, x, core), col: 2 (over y).
Axes of the slice: x: 2, y: 2, z: 4, core: 2. Of those that a mesh axis runs over, the one named last changes fastest.
Arguments:
- embed_first: bfloat16 [768, 16384], P('col', 'row'), may hold values from -6 to 6
- embed_second: bfloat16 [768, 16384], P('row', 'col'), may hold values from -6 to 6
- corr_grad: float32 [16384, 16384], P('row', 'col'), may hold values from -0.046875 to 0.046875
Outputs:
- grad_first: bfloat16 [768, 16384], P('col', 'row')
- grad_second: bfloat16 [768, 16384], P('row', 'col')
The draws below stay inside these ranges and needn't reach their ends.
All inputs are finite; a program needn't handle non-finite values.
Results may differ from the reference program's by a relative error of at most 0.0065.
Values may be sent and summed in bfloat16 or wider, within the bound.
A program may use at most 128 MiB of HBM per device.

```python
import jax
import jax.numpy as jnp
from jax import lax

F = 16384
BATCH = 768


def levels(key, extent, cuts, low, high):
    def one(axis_at, shards_of):
        draws = jax.random.uniform(jax.random.fold_in(jax.random.fold_in(key, 6), axis_at), (shards_of,), jnp.float32, low / len(cuts), high / len(cuts))
        return jnp.repeat(jnp.exp(draws), extent[axis_at] // shards_of).reshape((-1,) + (1,) * (len(extent) - axis_at - 1))

    loudness = one(*cuts[0])
    for cut in cuts[1:]:
        loudness = loudness * one(*cut)
    return loudness


def noise(rng, shape, spread, limit, split=(), kind=jnp.bfloat16):
    gain = levels(rng, shape, split, -0.22, 0.18) if split else 1.0
    drawn = jax.random.normal(rng, shape, jnp.float32) * spread * gain
    return jnp.minimum(jnp.maximum(drawn, -limit), limit).astype(kind)


def setup_inputs(seed: int = 0) -> dict:
    splits = jax.random.split(jax.random.key(seed), 4)
    embed_first = noise(splits[0], (BATCH, F), 1.0, 6.0, ((0, 2), (1, 16)))
    embed_second = noise(splits[1], (BATCH, F), 1.0, 6.0, ((0, 16), (1, 2)))
    corr_grad = noise(splits[2], (F, F), F ** -0.5, 0.046875, ((0, 16), (1, 2)), jnp.float32)
    return {"embed_first": embed_first, "embed_second": embed_second, "corr_grad": corr_grad}


def reference(embed_first, embed_second, corr_grad):
    low_grad = corr_grad.astype(jnp.bfloat16)
    grad_first = lax.dot_general(embed_second, low_grad, (((1,), (1,)), ((), ())), preferred_element_type=jnp.float32)
    grad_second = jnp.dot(embed_first, low_grad, preferred_element_type=jnp.float32)
    return grad_first.astype(jnp.bfloat16), grad_second.astype(jnp.bfloat16)
```

```python
import functools

import jax
import jax.numpy as jnp
from jax import lax
from jax.experimental import pallas as pl
from jax.experimental.pallas import tpu as pltpu
from jax.sharding import PartitionSpec as P

PIECES = 4
TILE = 256
SLOTS = 3
EARLY = 3


def kernel(
    a_side, b_side, cols, early,
    e1_ref, e2_ref, g_ref, o1_ref, o2_ref,
    e1x, e2x, gb, p2, s2, rb, t1s, t1r, gt,
    g_sem, e1_send, e1_recv, ag_send, ag_recv, sib_send, sib_recv,
    d2d_send, d2d_recv, rs_send, rs_recv, t1_send, t1_recv,
):
    chips = a_side * b_side
    block, fj = e2_ref.shape
    rows, fi = e1_ref.shape
    share = chips // cols
    width = fj // PIECES
    half = PIECES // 2
    bf16, f32 = jnp.bfloat16, jnp.float32

    me = lax.axis_index("row")
    my_col = lax.axis_index("col")
    chip, core = me // 2, me % 2
    other = 1 - core

    def chip_at(pos):
        first = 1 - jnp.minimum(pos // a_side, 1)
        q = jnp.maximum(pos - a_side, 0)
        i, j = q // (b_side - 1), q % (b_side - 1)
        odd = i % 2
        b = (1 - odd) * (1 + j) + odd * (b_side - 1 - j)
        return first * (pos * b_side) + (1 - first) * ((a_side - 1 - i) * b_side + b)

    a, b = chip // b_side, chip % b_side
    i = a_side - 1 - a
    later = a_side + i * (b_side - 1) + (1 - i % 2) * (b - 1) + (i % 2) * (b_side - 1 - b)
    inner = jnp.minimum(b, 1)
    pos = (1 - inner) * a + inner * later

    def chip_off(offset):
        return chip_at((pos + offset + 2 * chips) % chips)

    right = chip_off(1) * 2 + core
    left = chip_off(-1) * 2 + core
    sibling = chip * 2 + other

    def piece(k):
        return pl.ds(k * width, width)

    def ahead(k):
        return right if k < half else left

    def sign(k):
        return 1 if k < half else -1

    def remote(src, dst, send, recv, **to):
        return pltpu.make_async_remote_copy(
            src_ref=src, dst_ref=dst, send_sem=send, recv_sem=recv,
            device_id=to, device_id_type=pl.DeviceIdType.MESH,
        )

    barrier = pltpu.get_barrier_semaphore()
    for to in (right, left, sibling):
        pl.semaphore_signal(barrier, inc=1, device_id={"row": to}, device_id_type=pl.DeviceIdType.MESH)
    for off in range(1, cols):
        pl.semaphore_signal(
            barrier, inc=1, device_id={"col": (my_col + off) % cols}, device_id_type=pl.DeviceIdType.MESH
        )
    pl.semaphore_wait(barrier, 3 + cols - 1)

    def gather_copy(t, k, first=False):
        src_chip = chip_off(-sign(k) * t)
        dst = e2x.at[src_chip, core, :, piece(k)]
        src = e2_ref.at[:, piece(k)] if first else dst
        return remote(src, dst, ag_send.at[t, k], ag_recv.at[t, k], row=ahead(k))

    def sibling_copy(t, k, first=False):
        src_chip = chip_off(-sign(k) * t)
        dst = e2x.at[src_chip, core, :, piece(k)]
        src = e2_ref.at[:, piece(k)] if first else dst
        return remote(src, dst, sib_send.at[t, k], sib_recv.at[t, k], row=sibling)

    def gather_step(t, last=False):
        for k in range(PIECES):
            gather_copy(t, k).wait_recv()
            if not last:
                gather_copy(t + 1, k).start()
            sibling_copy(t + 1, k).start()

    order = [k for pair in zip(range(half), range(half, PIECES)) for k in pair]
    for k in order:
        gather_copy(0, k, True).start()
    e1_copies = []
    for off in range(1, cols):
        to = (my_col + off) % cols
        e1_copies.append(remote(e1_ref, e1x.at[off - 1], e1_send.at[off - 1], e1_recv.at[off - 1], col=to))
        e1_copies[-1].start()

    def load(n):
        slot = n % SLOTS
        return pltpu.make_async_copy(
            g_ref.at[:, pl.ds(pl.multiple_of(n * TILE, TILE), TILE)], gt.at[slot], g_sem.at[slot]
        )

    tiles = fj // TILE
    for n in range(SLOTS):
        load(n).start()
    for k in order:
        sibling_copy(0, k, True).start()

    def first_pass(n, carry):
        load(n).wait()
        at = pl.ds(pl.multiple_of(n * TILE, TILE), TILE)
        low = gt[n % SLOTS].astype(bf16)
        gb[:, at] = low

        @pl.when(n + SLOTS < tiles)
        def _():
            load(n + SLOTS).start()

        terms = jnp.dot(e1_ref[...], low, preferred_element_type=f32).astype(bf16)
        p2[pl.ds(my_col * share, share), :, :, at] = terms.reshape(share, 2, block, TILE)
        return carry

    def next_pass(off, wide):
        from_col = (my_col - off + cols) % cols

        def body(n, carry):
            at = pl.ds(pl.multiple_of(n * wide, wide), wide)
            terms = jnp.dot(e1x[off - 1], gb[:, at], preferred_element_type=f32).astype(bf16)
            p2[pl.ds(from_col * share, share), :, :, at] = terms.reshape(share, 2, block, wide)
            return carry

        return body

    def d2d_copy(off, h):
        from_chip = pl.ds((my_col - off + cols) % cols * share, share)
        at = pl.ds(h * (fj // 2), fj // 2)
        return remote(
            p2.at[from_chip, other, :, at], s2.at[from_chip, :, at],
            d2d_send.at[off, h], d2d_recv.at[off, h], row=sibling,
        )

    taken = 0
    for h in range(2):
        lax.fori_loop(h * tiles // 2, (h + 1) * tiles // 2, first_pass, 0)
        d2d_copy(0, h).start()
    gather_step(taken)
    taken += 1
    e2x[chip, core] = e2_ref[...]
    wide = 512
    for off in range(1, cols):
        e1_copies[off - 1].wait_recv()
        for h in range(2):
            lax.fori_loop(h * fj // wide // 2, (h + 1) * fj // wide // 2, next_pass(off, wide), 0)
            d2d_copy(off, h).start()
        if taken < early:
            gather_step(taken)
            taken += 1
    while taken < early:
        gather_step(taken)
        taken += 1
    for off in range(cols):
        for h in range(2):
            d2d_copy(off, h).wait_recv()

    def sum_copy(t, k):
        to_chip = chip_off(-sign(k) * (t + 1))
        return remote(
            p2.at[to_chip, core, :, piece(k)], rb.at[t, :, piece(k)],
            rs_send.at[t, k], rs_recv.at[t, k], row=ahead(k),
        )

    def sum_first():
        for k in order:
            to_chip = chip_off(-sign(k))
            at = piece(k)
            total = p2[to_chip, core, :, at].astype(f32) + s2[to_chip, :, at].astype(f32)
            p2[to_chip, core, :, at] = total.astype(bf16)
            sum_copy(0, k).start()

    def sum_step(t):
        for k in order:
            to_chip = chip_off(-sign(k) * (t + 1))
            at = piece(k)
            sum_copy(t - 1, k).wait_recv()
            total = p2[to_chip, core, :, at].astype(f32) + s2[to_chip, :, at].astype(f32)
            total += rb[t - 1, :, at].astype(f32)
            p2[to_chip, core, :, at] = total.astype(bf16)
            sum_copy(t, k).start()

    sum_first()
    steps = chips - 1

    def both(t, carry):
        gather_step(t + early - 1)
        sum_step(t)
        return carry

    lax.fori_loop(1, steps - early, both, 0)
    done = steps - early
    gather_step(steps - 1, last=True)
    sum_step(done)
    done += 1
    for t in range(chips):
        for k in range(PIECES):
            sibling_copy(t, k).wait_recv()

    def t1_copy(off):
        return remote(
            t1s.at[off - 1], t1r.at[off - 1], t1_send.at[off - 1], t1_recv.at[off - 1],
            col=(my_col + off) % cols,
        )

    def first_terms(of_col, n):
        left_side = e2x[pl.ds(of_col * share, share)].reshape(rows, fj)
        part = gb[pl.ds(pl.multiple_of(n * TILE, TILE), TILE), :]
        return lax.dot_general(left_side, part, (((1,), (1,)), ((), ())), preferred_element_type=f32)

    for off in range(1, cols):
        def send_body(n, carry, off=off):
            at = pl.ds(pl.multiple_of(n * TILE, TILE), TILE)
            t1s[off - 1, :, at] = first_terms((my_col + off) % cols, n).astype(bf16)
            return carry

        lax.fori_loop(0, fi // TILE, send_body, 0)
        t1_copy(off).start()
        if done < steps:
            sum_step(done)
            done += 1

    def keep(n):
        return gt.at[n // 2, pl.ds(pl.multiple_of(n % 2 * rows, rows), rows)]

    def own_body(n, carry):
        keep(n)[...] = first_terms(my_col, n)
        return carry

    lax.fori_loop(0, fi // TILE, own_body, 0)
    while done < steps:
        sum_step(done)
        done += 1

    for off in range(1, cols):
        t1_copy(off).wait_recv()

    def out_body(n, carry):
        at = pl.ds(pl.multiple_of(n * TILE, TILE), TILE)
        total = keep(n)[...]
        for off in range(1, cols):
            total += t1r[off - 1, :, at].astype(f32)
        o1_ref[:, at] = total.astype(bf16)
        return carry

    lax.fori_loop(0, fi // TILE, out_body, 0)

    for k in order:
        at = piece(k)
        sum_copy(steps - 1, k).wait_recv()
        total = p2[chip, core, :, at].astype(f32) + s2[chip, :, at].astype(f32)
        o2_ref[:, at] = (total + rb[steps - 1, :, at].astype(f32)).astype(bf16)

    for t in range(steps):
        for k in range(PIECES):
            gather_copy(t, k).wait_send()
            sum_copy(t, k).wait_send()
    for t in range(chips):
        for k in range(PIECES):
            sibling_copy(t, k).wait_send()
    for off in range(cols):
        for h in range(2):
            d2d_copy(off, h).wait_send()
    for off in range(1, cols):
        e1_copies[off - 1].wait_send()
        t1_copy(off).wait_send()


def local(rows_size, cols, e1, e2, g):
    chips = rows_size // 2
    a_side = 4
    b_side = chips // a_side
    block, fj = e2.shape
    rows, fi = e1.shape
    bf16 = jnp.bfloat16
    vmem = pl.BlockSpec(memory_space=pltpu.VMEM)
    dma = pltpu.SemaphoreType.DMA
    steps = chips - 1
    return pl.pallas_call(
        functools.partial(kernel, a_side, b_side, cols, min(EARLY, steps - 2)),
        out_shape=(jax.ShapeDtypeStruct(e1.shape, bf16), jax.ShapeDtypeStruct(e2.shape, bf16)),
        in_specs=[vmem, vmem, pl.BlockSpec(memory_space=pl.ANY)],
        out_specs=(vmem, vmem),
        scratch_shapes=[
            pltpu.VMEM((cols - 1, rows, fi), bf16),
            pltpu.VMEM((chips, 2, block, fj), bf16),
            pltpu.VMEM((fi, fj), bf16),
            pltpu.VMEM((chips, 2, block, fj), bf16),
            pltpu.VMEM((chips, block, fj), bf16),
            pltpu.VMEM((steps, block, fj), bf16),
            pltpu.VMEM((cols - 1, rows, fi), bf16),
            pltpu.VMEM((cols - 1, rows, fi), bf16),
            pltpu.VMEM((SLOTS, fi, TILE), jnp.float32),
            dma((SLOTS,)),
            dma((cols - 1,)), dma((cols - 1,)),
            dma((steps, PIECES)), dma((steps, PIECES)),
            dma((chips, PIECES)), dma((chips, PIECES)),
            dma((cols, 2)), dma((cols, 2)),
            dma((steps, PIECES)), dma((steps, PIECES)),
            dma((cols - 1,)), dma((cols - 1,)),
        ],
        compiler_params=pltpu.CompilerParams(
            collective_id=0, has_side_effects=True, vmem_limit_bytes=67043328
        ),
    )(e1, e2, g)


def solution(mesh):
    return jax.shard_map(
        functools.partial(local, mesh.shape["row"], mesh.shape["col"]),
        mesh=mesh,
        in_specs=(P("col", "row"), P("row", "col"), P("row", "col")),
        out_specs=(P("col", "row"), P("row", "col")),
        check_vma=False,
    )
```

```python
import functools

import jax
import jax.numpy as jnp
from jax import lax
from jax.experimental import pallas as pl
from jax.experimental.pallas import tpu as pltpu
from jax.sharding import PartitionSpec as P

FIRST_SHARE = 0.4
TILE = 256
SLOTS = 3


def cuts(fj):
    unit = fj // 256
    short = round(unit * FIRST_SHARE)
    widths = [(True, short), (True, short), (False, unit - short), (False, unit - short)]
    out, at = [], 0
    for kind, w in widths:
        out.append((kind, at, w * 128))
        at += w * 128
    return out


def slots_of(side):
    return 1 if side == 2 else side + 1


def kernel(
    a_side, b_side, cols,
    e1_ref, e2_ref, g_ref, o1_ref, o2_ref,
    e1x, e2x, gb, p2, s2, rb_short, rb_long, acc, t1s, t1r, gt,
    g_sem, e1_send, e1_recv, ag_send, ag_recv, sib_send, sib_recv,
    d2d_send, d2d_recv, rs_send, rs_recv_short, rs_recv_long, t1_send, t1_recv,
):
    chips = a_side * b_side
    block, fj = e2_ref.shape
    rows, fi = e1_ref.shape
    share = chips // cols
    bf16, f32 = jnp.bfloat16, jnp.float32
    pieces = cuts(fj)
    order = [2, 0, 3, 1]
    sides = {"a": a_side, "b": b_side}

    me = lax.axis_index("row")
    my_col = lax.axis_index("col")
    chip, core = me // 2, me % 2
    other = 1 - core
    here = {"a": chip // b_side, "b": chip % b_side}
    sibling = chip * 2 + other

    def at_offset(da, db):
        return chip + da * b_side + db

    def neighbour(axis, sign):
        return (chip + sign * (b_side if axis == "a" else 1)) * 2 + core

    def inside(axis, d):
        where = here[axis] + d
        return jnp.logical_and(where >= 0, where < sides[axis])

    def both_inside(da, db):
        return jnp.logical_and(inside("a", da), inside("b", db))

    def offsets(distance):
        for da in range(a_side - 1, -a_side, -1):
            for db in range(b_side - 1, -b_side, -1):
                if abs(da) + abs(db) == distance:
                    yield da, db

    far = a_side + b_side - 2

    def piece(k):
        return pl.ds(pieces[k][1], pieces[k][2])

    def remote(src, dst, send, recv, **to):
        return pltpu.make_async_remote_copy(
            src_ref=src, dst_ref=dst, send_sem=send, recv_sem=recv,
            device_id=to, device_id_type=pl.DeviceIdType.MESH,
        )

    WAYS = (("a", 1), ("a", -1), ("b", 1), ("b", -1))

    barrier = pltpu.get_barrier_semaphore()
    for axis, sign in WAYS:
        @pl.when(inside(axis, sign))
        def _():
            pl.semaphore_signal(
                barrier, inc=1, device_id={"row": neighbour(axis, sign)}, device_id_type=pl.DeviceIdType.MESH
            )
    pl.semaphore_signal(barrier, inc=1, device_id={"row": sibling}, device_id_type=pl.DeviceIdType.MESH)
    for off in range(1, cols):
        pl.semaphore_signal(
            barrier, inc=1, device_id={"col": (my_col + off) % cols}, device_id_type=pl.DeviceIdType.MESH
        )
    peers = sum(inside(*way).astype(jnp.int32) for way in WAYS)
    pl.semaphore_wait(barrier, peers + cols)

    def block_copy(da, db, k, way):
        src_chip = at_offset(da, db)
        dst = e2x.at[src_chip, core, :, piece(k)]
        src = e2_ref.at[:, piece(k)] if (da, db) == (0, 0) else dst
        return remote(
            src, dst, ag_send.at[src_chip, k, way], ag_recv.at[src_chip, k], row=neighbour(*WAYS[way])
        )

    def sibling_copy(da, db, k):
        src_chip = at_offset(da, db)
        dst = e2x.at[src_chip, core, :, piece(k)]
        src = e2_ref.at[:, piece(k)] if (da, db) == (0, 0) else dst
        return remote(src, dst, sib_send.at[src_chip, k], sib_recv.at[src_chip, k], row=sibling)

    def onward(da, db, k):
        first, second = ("b", "a") if pieces[k][0] else ("a", "b")
        d = {"a": da, "b": db}
        for way, (axis, sign) in enumerate(WAYS):
            if axis == second:
                if d[second] * sign <= 0:
                    yield way
            elif d[second] == 0 and d[first] * sign <= 0:
                yield way

    def send_on(da, db, k):
        for way in onward(da, db, k):
            @pl.when(inside(*WAYS[way]))
            def _():
                block_copy(da, db, k, way).start()

    def gather_round(distance):
        for da, db in offsets(distance):
            @pl.when(both_inside(da, db))
            def _():
                for k in order:
                    block_copy(da, db, k, 0).wait_recv()
                    send_on(da, db, k)
                    sibling_copy(da, db, k).start()

    for k in order:
        send_on(0, 0, k)
    e1_copies = []
    for off in range(1, cols):
        to = (my_col + off) % cols
        e1_copies.append(remote(e1_ref, e1x.at[off - 1], e1_send.at[off - 1], e1_recv.at[off - 1], col=to))
        e1_copies[-1].start()

    def load(n):
        slot = n % SLOTS
        return pltpu.make_async_copy(
            g_ref.at[:, pl.ds(pl.multiple_of(n * TILE, TILE), TILE)], gt.at[slot], g_sem.at[slot]
        )

    tiles = fj // TILE
    for n in range(SLOTS):
        load(n).start()
    for k in order:
        sibling_copy(0, 0, k).start()

    def first_pass(n, carry):
        load(n).wait()
        at = pl.ds(pl.multiple_of(n * TILE, TILE), TILE)
        low = gt[n % SLOTS].astype(bf16)
        gb[:, at] = low

        @pl.when(n + SLOTS < tiles)
        def _():
            load(n + SLOTS).start()

        terms = jnp.dot(e1_ref[...], low, preferred_element_type=f32).astype(bf16)
        p2[pl.ds(my_col * share, share), :, :, at] = terms.reshape(share, 2, block, TILE)
        return carry

    def next_pass(off, wide):
        from_col = (my_col - off + cols) % cols

        def body(n, carry):
            at = pl.ds(pl.multiple_of(n * wide, wide), wide)
            terms = jnp.dot(e1x[off - 1], gb[:, at], preferred_element_type=f32).astype(bf16)
            p2[pl.ds(from_col * share, share), :, :, at] = terms.reshape(share, 2, block, wide)
            return carry

        return body

    def d2d_copy(off, h):
        from_chip = pl.ds((my_col - off + cols) % cols * share, share)
        at = pl.ds(h * (fj // 2), fj // 2)
        return remote(
            p2.at[from_chip, other, :, at], s2.at[from_chip, :, at],
            d2d_send.at[off, h], d2d_recv.at[off, h], row=sibling,
        )

    for h in range(2):
        lax.fori_loop(h * tiles // 2, (h + 1) * tiles // 2, first_pass, 0)
        d2d_copy(0, h).start()
    gather_round(1)
    e2x[chip, core] = e2_ref[...]
    wide = 512
    for off in range(1, cols):
        e1_copies[off - 1].wait_recv()
        for h in range(2):
            lax.fori_loop(h * fj // wide // 2, (h + 1) * fj // wide // 2, next_pass(off, wide), 0)
            d2d_copy(off, h).start()
    for off in range(cols):
        for h in range(2):
            d2d_copy(off, h).wait_recv()

    def sum_slot(k, axis, sign, to):
        short = pieces[k][0]
        first, second = ("a", "b") if short else ("b", "a")
        place = to["a"] if axis == "a" else to["b"]
        slot = 0 if sides[axis] == 2 else (place + 1 if sign > 0 else place)
        if axis == first:
            slot = to[second] * slots_of(sides[first]) + slot
        else:
            slot = sides[second] * slots_of(sides[first]) + slot
        start = pieces[k][1] if short else pieces[k][1] - pieces[2][1]
        buf = rb_short if short else rb_long
        sem = rs_recv_short if short else rs_recv_long
        return buf.at[slot, :, pl.ds(start, pieces[k][2])], sem.at[slot, k % 2]

    def place_of(da, db):
        return {"a": here["a"] + da, "b": here["b"] + db}

    def way_out(da, db, k):
        first, second = ("a", "b") if pieces[k][0] else ("b", "a")
        d = {"a": da, "b": db}
        axis = first if d[first] else second
        return axis, (1 if d[axis] > 0 else -1)

    def sum_copy(da, db, k):
        axis, sign = way_out(da, db, k)
        to_chip = at_offset(da, db)
        dst, sem = sum_slot(k, axis, sign, place_of(da, db))
        return remote(
            p2.at[to_chip, core, :, piece(k)], dst, rs_send.at[to_chip, k], sem, row=neighbour(axis, sign)
        )

    def arrivals(da, db, k):
        first, second = ("a", "b") if pieces[k][0] else ("b", "a")
        d = {"a": da, "b": db}
        out = []
        for sign in (1, -1):
            if d[first] * sign >= 0:
                out.append((first, sign))
        if d[first] == 0:
            for sign in (1, -1):
                if d[second] * sign >= 0:
                    out.append((second, sign))
        return out

    def sum_of(da, db, k):
        at = piece(k)
        to_chip = at_offset(da, db)
        kept = acc.at[:, pl.ds(0, pieces[k][2])]
        kept[...] = p2[to_chip, core, :, at].astype(f32) + s2[to_chip, :, at].astype(f32)
        for axis, sign in arrivals(da, db, k):
            @pl.when(inside(axis, -sign))
            def _():
                buf, sem = sum_slot(k, axis, sign, place_of(da, db))
                remote(buf, buf, rs_send.at[0, k], sem, row=sibling).wait_recv()
                kept[...] += buf[...].astype(f32)
        return kept[...].astype(bf16)

    def sum_round(distance):
        for da, db in offsets(distance):
            @pl.when(both_inside(da, db))
            def _():
                for k in order:
                    p2[at_offset(da, db), core, :, piece(k)] = sum_of(da, db, k)
                    sum_copy(da, db, k).start()

    left_to_sum = list(range(far, 0, -1))
    for distance in range(2, far + 1):
        sum_round(left_to_sum.pop(0))
        gather_round(distance)
    for da in range(1 - a_side, a_side):
        for db in range(1 - b_side, b_side):
            @pl.when(both_inside(da, db))
            def _():
                for k in range(4):
                    sibling_copy(da, db, k).wait_recv()

    def t1_copy(off):
        return remote(
            t1s.at[off - 1], t1r.at[off - 1], t1_send.at[off - 1], t1_recv.at[off - 1],
            col=(my_col + off) % cols,
        )

    def first_terms(of_col, n):
        left_side = e2x[pl.ds(of_col * share, share)].reshape(rows, fj)
        part = gb[pl.ds(pl.multiple_of(n * TILE, TILE), TILE), :]
        return lax.dot_general(left_side, part, (((1,), (1,)), ((), ())), preferred_element_type=f32)

    for off in range(1, cols):
        def send_body(n, carry, off=off):
            at = pl.ds(pl.multiple_of(n * TILE, TILE), TILE)
            t1s[off - 1, :, at] = first_terms((my_col + off) % cols, n).astype(bf16)
            return carry

        lax.fori_loop(0, fi // TILE, send_body, 0)
        t1_copy(off).start()
        if left_to_sum:
            sum_round(left_to_sum.pop(0))

    def keep(n):
        return gt.at[n // 2, pl.ds(pl.multiple_of(n % 2 * rows, rows), rows)]

    def own_body(n, carry):
        keep(n)[...] = first_terms(my_col, n)
        return carry

    lax.fori_loop(0, fi // TILE, own_body, 0)
    while left_to_sum:
        sum_round(left_to_sum.pop(0))

    for off in range(1, cols):
        t1_copy(off).wait_recv()

    def out_body(n, carry):
        at = pl.ds(pl.multiple_of(n * TILE, TILE), TILE)
        total = keep(n)[...]
        for off in range(1, cols):
            total += t1r[off - 1, :, at].astype(f32)
        o1_ref[:, at] = total.astype(bf16)
        return carry

    lax.fori_loop(0, fi // TILE, out_body, 0)

    for k in order:
        o2_ref[:, piece(k)] = sum_of(0, 0, k)

    for da in range(1 - a_side, a_side):
        for db in range(1 - b_side, b_side):
            @pl.when(both_inside(da, db))
            def _():
                for k in range(4):
                    for way in onward(da, db, k):
                        @pl.when(inside(*WAYS[way]))
                        def _():
                            block_copy(da, db, k, way).wait_send()
                    sibling_copy(da, db, k).wait_send()
                    if (da, db) != (0, 0):
                        sum_copy(da, db, k).wait_send()
    for off in range(cols):
        for h in range(2):
            d2d_copy(off, h).wait_send()
    for off in range(1, cols):
        e1_copies[off - 1].wait_send()
        t1_copy(off).wait_send()


def local(rows_size, cols, e1, e2, g):
    chips = rows_size // 2
    a_side = 4
    b_side = chips // a_side
    block, fj = e2.shape
    rows, fi = e1.shape
    bf16 = jnp.bfloat16
    vmem = pl.BlockSpec(memory_space=pltpu.VMEM)
    dma = pltpu.SemaphoreType.DMA
    pieces = cuts(fj)
    short, long = 2 * pieces[0][2], 2 * pieces[2][2]
    short_slots = b_side * slots_of(a_side) + slots_of(b_side)
    long_slots = a_side * slots_of(b_side) + slots_of(a_side)
    return pl.pallas_call(
        functools.partial(kernel, a_side, b_side, cols),
        out_shape=(jax.ShapeDtypeStruct(e1.shape, bf16), jax.ShapeDtypeStruct(e2.shape, bf16)),
        in_specs=[vmem, vmem, pl.BlockSpec(memory_space=pl.ANY)],
        out_specs=(vmem, vmem),
        scratch_shapes=[
            pltpu.VMEM((cols - 1, rows, fi), bf16),
            pltpu.VMEM((chips, 2, block, fj), bf16),
            pltpu.VMEM((fi, fj), bf16),
            pltpu.VMEM((chips, 2, block, fj), bf16),
            pltpu.VMEM((chips, block, fj), bf16),
            pltpu.VMEM((short_slots, block, short), bf16),
            pltpu.VMEM((long_slots, block, long), bf16),
            pltpu.VMEM((block, max(short, long) // 2), jnp.float32),
            pltpu.VMEM((cols - 1, rows, fi), bf16),
            pltpu.VMEM((cols - 1, rows, fi), bf16),
            pltpu.VMEM((SLOTS, fi, TILE), jnp.float32),
            dma((SLOTS,)),
            dma((cols - 1,)), dma((cols - 1,)),
            dma((chips, 4, 4)), dma((chips, 4)),
            dma((chips, 4)), dma((chips, 4)),
            dma((cols, 2)), dma((cols, 2)),
            dma((chips, 4)), dma((short_slots, 2)), dma((long_slots, 2)),
            dma((cols - 1,)), dma((cols - 1,)),
        ],
        compiler_params=pltpu.CompilerParams(
            collective_id=0, has_side_effects=True, vmem_limit_bytes=67043328
        ),
    )(e1, e2, g)


def solution(mesh):
    return jax.shard_map(
        functools.partial(local, mesh.shape["row"], mesh.shape["col"]),
        mesh=mesh,
        in_specs=(P("col", "row"), P("row", "col"), P("row", "col")),
        out_specs=(P("col", "row"), P("row", "col")),
        check_vma=False,
    )
```
